16 devices in a mesh: tp: 2 (over z), dp: 8 (over y, x, core).
Axes of the slice: x: 2, y: 2, z: 2, core: 2. Of those that a mesh axis runs over, the one named last changes fastest.
Arguments:
- hidden: bfloat16 [8192, 960], P('dp')
- norm_w: bfloat16 [960], replicated
- emb_table: bfloat16 [49152, 960], P('tp')
- teacher: bfloat16 [8192, 49152], P('dp', 'tp')
- loss_mask: int32 [8192], P('dp')
Outputs:
- output 1: float32 [], replicated
- output 2: bfloat16 [8192, 960], P('dp')
- output 3: float32 [49152, 960], P('tp', 'dp')
- output 4: float32 [960], replicated
All inputs are finite; a program needn't handle non-finite values.
Results may differ from the reference program's by a relative error of at most 0.00103912.
Values sent between devices are 32-bit elements.
A program may use at most 1 GiB of HBM per device.

```python
import jax
import jax.numpy as jnp
from jax import lax

MODEL_DIM = 960
VOCAB_SIZE = 49152
TOK_DEV = 1024
DP_SHARDS = 8
TOKENS = TOK_DEV * DP_SHARDS
SOFT_CAP = 30.0
NORM_EPS = 1e-6


def setup_inputs(seed: int = 0) -> dict:
    base_key = jax.random.key(seed)
    key_list = jax.random.split(base_key, 6)
    hidden = jax.random.normal(key_list[0], (TOKENS, MODEL_DIM), jnp.float32)
    norm_w = 0.5 * jax.random.normal(key_list[1], (MODEL_DIM,), jnp.float32)
    mean_dir = jax.random.normal(key_list[2], (MODEL_DIM,), jnp.float32)
    emb_noise = jax.random.normal(key_list[3], (VOCAB_SIZE, MODEL_DIM), jnp.float32)
    emb_table = (18.0 * mean_dir[None, :] + 1.5 * emb_noise) * (MODEL_DIM ** -0.5)
    teacher = 2.0 * jax.random.normal(key_list[4], (TOKENS, VOCAB_SIZE), jnp.float32)
    lengths = jax.random.randint(key_list[5], (DP_SHARDS,), 1, TOK_DEV + 1)
    lengths = jnp.where(jnp.arange(DP_SHARDS) == 0, TOK_DEV, lengths)
    loss_mask = (jnp.arange(TOK_DEV)[None, :] < lengths[:, None]).astype(jnp.int32)
    return {'hidden': hidden.astype(jnp.bfloat16), 'norm_w': norm_w.astype(jnp.bfloat16), 'emb_table': emb_table.astype(jnp.bfloat16), 'teacher': teacher.astype(jnp.bfloat16), 'loss_mask': loss_mask.reshape(TOKENS)}


def rms_norm(hid_f32, scale_f32):
    inv_rms = lax.rsqrt(jnp.mean(hid_f32 * hid_f32, axis=-1, keepdims=True) + NORM_EPS)
    return hid_f32 * inv_rms * (1.0 + scale_f32)


def reference(hidden, norm_w, emb_table, teacher, loss_mask):
    mask_f32 = loss_mask.astype(jnp.float32)
    weights = mask_f32 / jnp.sum(mask_f32)
    scale_f32 = norm_w.astype(jnp.float32)

    def block_step(acc_state, blk_inputs):
        emb_acc, scale_acc = acc_state
        hid_blk, teach_blk, weight_blk = blk_inputs
        normed_f32, norm_pull = jax.vjp(rms_norm, hid_blk.astype(jnp.float32), scale_f32)
        normed = normed_f32.astype(jnp.bfloat16)
        raw_logit = jnp.dot(normed, emb_table.T, preferred_element_type=jnp.float32)
        tanh_val = jnp.tanh(raw_logit / SOFT_CAP)
        capped = SOFT_CAP * tanh_val
        log_stu = jax.nn.log_softmax(capped, axis=-1)
        log_tea = jax.nn.log_softmax(teach_blk.astype(jnp.float32), axis=-1)
        prob_tea = jnp.exp(log_tea)
        kl_tok = jnp.sum(prob_tea * (log_tea - log_stu), axis=-1)
        loss_part = jnp.sum(weight_blk * kl_tok)
        d_raw = ((jnp.exp(log_stu) - prob_tea) * weight_blk[:, None] * (1.0 - tanh_val * tanh_val)).astype(jnp.bfloat16)
        grad_normed = jnp.dot(d_raw, emb_table, preferred_element_type=jnp.float32)
        emb_acc = emb_acc + jnp.dot(d_raw.T, normed, preferred_element_type=jnp.float32)
        grad_hid, grad_scale = norm_pull(grad_normed)
        return (emb_acc, scale_acc + grad_scale), (loss_part, grad_hid.astype(jnp.bfloat16))

    blocks_in = (hidden.reshape(DP_SHARDS, TOK_DEV, MODEL_DIM), teacher.reshape(DP_SHARDS, TOK_DEV, VOCAB_SIZE), weights.reshape(DP_SHARDS, TOK_DEV))
    start_acc = (jnp.zeros((VOCAB_SIZE, MODEL_DIM), jnp.float32), jnp.zeros((MODEL_DIM,), jnp.float32))
    final_acc, per_block = lax.scan(block_step, start_acc, blocks_in)
    d_emb, d_norm_w = final_acc
    loss_parts, grad_hid = per_block
    return jnp.sum(loss_parts), grad_hid.reshape(TOKENS, MODEL_DIM), d_emb, d_norm_w
```

```python
import functools

import jax
import jax.numpy as jnp
from jax import lax
from jax.experimental import pallas as pl
from jax.experimental.pallas import tpu as pltpu
from jax.sharding import PartitionSpec as P


SOFT_CAP = 30.0
NORM_EPS = 1e-6
LOG2E = 1.4426950408889634
TILE = 512
STRIP = 256
SUB = 16
LANES = 128
CHUNK_TILES = (2, 6, 10, 12, 10, 6, 2)
LOWEST = -3.0e38
VMEM_LIMIT = 60 * 1024 * 1024


def rms_norm(hid_f32, scale_f32):
    inv_rms = lax.rsqrt(jnp.mean(hid_f32 * hid_f32, axis=-1, keepdims=True) + NORM_EPS)
    return hid_f32 * inv_rms * (1.0 + scale_f32)


def params():
    return pltpu.CompilerParams(dimension_semantics=("arbitrary",), vmem_limit_bytes=VMEM_LIMIT)


def stats_kernel(steps, g_ref, e_ref, t_ref, out_ref, m_ref, zs_ref, zt_ref, kl_ref):
    step = pl.program_id(0)

    @pl.when(step == 0)
    def _():
        m_ref[...] = jnp.full(m_ref.shape, LOWEST, jnp.float32)
        zs_ref[...] = jnp.zeros_like(zs_ref)
        zt_ref[...] = jnp.zeros_like(zt_ref)
        kl_ref[...] = jnp.zeros_like(kl_ref)

    groups = TILE // LANES
    tokens = g_ref.shape[0]

    def logits(strip):
        return jnp.dot(g_ref[pl.ds(strip * STRIP, STRIP), :], e_ref[...], preferred_element_type=jnp.float32)

    raw = logits(0)
    for strip in range(tokens // STRIP):
        following = logits(strip + 1) if (strip + 1) * STRIP < tokens else None
        for sub in range(STRIP // SUB):
            rows = pl.ds(strip * STRIP + sub * SUB, SUB)
            block = raw[sub * SUB:(sub + 1) * SUB]
            tea = t_ref[rows, :].astype(jnp.float32)
            parts = [tea[:, k * LANES:(k + 1) * LANES] for k in range(groups)]
            top = m_ref[rows, :]
            old = top
            for part in parts:
                top = jnp.maximum(top, part)
            decay = jnp.exp2((old - top) * LOG2E)
            zs = zs_ref[rows, :]
            zt = zt_ref[rows, :] * decay
            kl = kl_ref[rows, :] * decay
            for k, part in enumerate(parts):
                tanh_val = jnp.tanh(block[:, k * LANES:(k + 1) * LANES] * (1.0 / SOFT_CAP))
                zs = zs + jnp.exp2(tanh_val * (SOFT_CAP * LOG2E))
                ex = jnp.exp2((part - top) * LOG2E)
                zt = zt + ex
                kl = kl + ex * (part - SOFT_CAP * tanh_val)
            m_ref[rows, :] = top
            zs_ref[rows, :] = zs
            zt_ref[rows, :] = zt
            kl_ref[rows, :] = kl
        raw = following

    @pl.when(step == steps - 1)
    def _():
        lane_max = m_ref[...]
        top = jnp.max(lane_max, axis=-1, keepdims=True)
        decay = jnp.exp2((lane_max - top) * LOG2E)
        zs = jnp.sum(zs_ref[...], axis=-1, keepdims=True)
        zt = jnp.sum(zt_ref[...] * decay, axis=-1, keepdims=True)
        kl = jnp.sum(kl_ref[...] * decay, axis=-1, keepdims=True)
        lane = lax.broadcasted_iota(jnp.int32, lane_max.shape, 1)
        packed = jnp.where(lane == 0, top, jnp.where(lane == 1, zs, jnp.where(lane == 2, zt, kl)))
        out_ref[...] = packed.T[:8, :]


def run_stats(normed, emb_t, teach):
    tokens, dim = normed.shape
    vocab = emb_t.shape[1]
    steps = vocab // TILE
    return pl.pallas_call(
        functools.partial(stats_kernel, steps),
        name="stats",
        grid=(steps,),
        out_shape=jax.ShapeDtypeStruct((8, tokens), jnp.float32),
        in_specs=[
            pl.BlockSpec((tokens, dim), lambda j: (0, 0)),
            pl.BlockSpec((dim, TILE), lambda j: (0, j)),
            pl.BlockSpec((tokens, TILE), lambda j: (0, j)),
        ],
        out_specs=pl.BlockSpec((8, tokens), lambda j: (0, 0)),
        scratch_shapes=[pltpu.VMEM((tokens, LANES), jnp.float32)] * 4,
        compiler_params=params(),
        cost_estimate=pl.CostEstimate(flops=2 * tokens * dim * vocab, bytes_accessed=2 * vocab * (tokens + dim), transcendentals=3 * tokens * vocab),
    )(normed, emb_t, teach)


def a_kernel(order_ref, prev_ref, coef_ref, g_ref, gp_ref, e_ref, t_ref, dr_ref, pp_ref, dg_ref, tok_ref):
    @pl.when(pl.program_id(0) == 0)
    def _():
        dg_ref[...] = prev_ref[...]
        tok_ref[...] = jnp.zeros_like(tok_ref)

    groups = TILE // LANES
    tokens = g_ref.shape[0]

    def logits(strip):
        return jnp.dot(g_ref[pl.ds(strip * STRIP, STRIP), :], e_ref[...], preferred_element_type=jnp.float32)

    raw = logits(0)
    for strip in range(tokens // STRIP):
        following = logits(strip + 1) if (strip + 1) * STRIP < tokens else None
        for sub in range(STRIP // SUB):
            rows = pl.ds(strip * STRIP + sub * SUB, SUB)
            block = raw[sub * SUB:(sub + 1) * SUB]
            tea = t_ref[rows, :].astype(jnp.float32)
            top = coef_ref[0, rows, :]
            stu_w = coef_ref[1, rows, :]
            tea_w = coef_ref[2, rows, :]
            for k in range(groups):
                cols = slice(k * LANES, (k + 1) * LANES)
                tanh_val = jnp.tanh(block[:, cols] * (1.0 / SOFT_CAP))
                stu = jnp.exp2(tanh_val * (SOFT_CAP * LOG2E)) * stu_w
                soft = jnp.exp2((tea[:, cols] - top) * LOG2E) * tea_w
                d_raw = (stu - soft) * (1.0 - tanh_val * tanh_val)
                dr_ref[rows, cols] = d_raw.astype(jnp.bfloat16)
        raw = following

    d_raw = dr_ref[...]
    pp_ref[...] = jnp.dot(gp_ref[0], d_raw, preferred_element_type=jnp.float32)
    dg_ref[...] += lax.dot_general(d_raw, e_ref[...], (((1,), (1,)), ((), ())), preferred_element_type=jnp.float32)


def run_a(first, tiles, order, prev, coef, normed, g_partner, emb_t, teach):
    tokens, dim = normed.shape
    half = tiles // 2
    width = tiles * TILE
    rows = g_partner.shape[1]
    return pl.pallas_call(
        a_kernel,
        name="dlogits",
        grid=(tiles,),
        out_shape=[
            jax.ShapeDtypeStruct((tokens, width), jnp.bfloat16),
            jax.ShapeDtypeStruct((rows, width), jnp.float32),
            jax.ShapeDtypeStruct((tokens, dim), jnp.float32),
            jax.ShapeDtypeStruct((8, LANES), jnp.float32),
        ],
        in_specs=[
            pl.BlockSpec((8, LANES), lambda j: (0, 0)),
            pl.BlockSpec((tokens, dim), lambda j: (0, 0)),
            pl.BlockSpec((3, tokens, LANES), lambda j: (0, 0, 0)),
            pl.BlockSpec((tokens, dim), lambda j: (0, 0)),
            pl.BlockSpec((1, rows, tokens), lambda j: (j // half, 0, 0)),
            pl.BlockSpec((dim, TILE), lambda j: (0, first + j)),
            pl.BlockSpec((tokens, TILE), lambda j: (0, first + j)),
        ],
        out_specs=[
            pl.BlockSpec((tokens, TILE), lambda j: (0, j)),
            pl.BlockSpec((rows, TILE), lambda j: (0, j)),
            pl.BlockSpec((tokens, dim), lambda j: (0, 0)),
            pl.BlockSpec((8, LANES), lambda j: (0, 0)),
        ],
        compiler_params=params(),
        cost_estimate=pl.CostEstimate(flops=5 * tokens * dim * width, bytes_accessed=10 * tokens * width, transcendentals=3 * tokens * width),
    )(order, prev, coef, normed, g_partner, emb_t, teach)


def b_kernel(half, order_ref, go_ref, dr_ref, r_ref, keep_ref, send0_ref, send1_ref, tok_ref):
    step = pl.program_id(0)
    total = jnp.dot(go_ref[0], dr_ref[...], preferred_element_type=jnp.float32) + r_ref[...]
    mid = keep_ref.shape[0]
    keep_ref[...] = total[:mid]

    @pl.when(step == 0)
    def _():
        tok_ref[...] = jnp.zeros_like(tok_ref)

    @pl.when(step < half)
    def _():
        send0_ref[...] = total[mid:]

    @pl.when(step >= half)
    def _():
        send1_ref[...] = total[mid:]


def run_b(tiles, order, g_own, d_raw, recv):
    tokens = d_raw.shape[0]
    rows = g_own.shape[1]
    half = tiles // 2
    width = tiles * TILE
    lower = lambda j: (0, jnp.minimum(j, half - 1))
    upper = lambda j: (0, jnp.maximum(j - half, 0))
    return pl.pallas_call(
        functools.partial(b_kernel, half),
        name="own_half",
        grid=(tiles,),
        out_shape=[
            jax.ShapeDtypeStruct((rows // 2, width), jnp.float32),
            jax.ShapeDtypeStruct((rows // 2, width // 2), jnp.float32),
            jax.ShapeDtypeStruct((rows // 2, width // 2), jnp.float32),
            jax.ShapeDtypeStruct((8, LANES), jnp.float32),
        ],
        in_specs=[
            pl.BlockSpec((8, LANES), lambda j: (0, 0)),
            pl.BlockSpec((1, rows, tokens), lambda j: (j // half, 0, 0)),
            pl.BlockSpec((tokens, TILE), lambda j: (0, j)),
            pl.BlockSpec((rows, TILE), lambda j: (0, j)),
        ],
        out_specs=[
            pl.BlockSpec((rows // 2, TILE), lambda j: (0, j)),
            pl.BlockSpec((rows // 2, TILE), lower),
            pl.BlockSpec((rows // 2, TILE), upper),
            pl.BlockSpec((8, LANES), lambda j: (0, 0)),
        ],
        compiler_params=params(),
        cost_estimate=pl.CostEstimate(flops=2 * tokens * rows * width, bytes_accessed=width * (2 * tokens + 8 * rows), transcendentals=0),
    )(order, g_own, d_raw, recv)


def relay_kernel(half, order_ref, keep_ref, rx_ref, ry_ref, last0_ref, last1_ref, tok_ref):
    step = pl.program_id(0)

    @pl.when(step == 0)
    def _():
        tok_ref[...] = jnp.zeros_like(tok_ref)

    @pl.when(step < half)
    def _():
        last0_ref[...] = keep_ref[...] + rx_ref[...]

    @pl.when(step >= half)
    def _():
        last1_ref[...] = keep_ref[...] + ry_ref[...]


def run_relay(tiles, order, keep, rx, ry):
    rows = keep.shape[0] // 2
    half = tiles // 2
    width = half * TILE
    lower = lambda j: jnp.minimum(j, half - 1)
    upper = lambda j: jnp.maximum(j - half, 0)
    return pl.pallas_call(
        functools.partial(relay_kernel, half),
        name="relay",
        grid=(tiles,),
        out_shape=[
            jax.ShapeDtypeStruct((rows, width), jnp.float32),
            jax.ShapeDtypeStruct((rows, width), jnp.float32),
            jax.ShapeDtypeStruct((8, LANES), jnp.float32),
        ],
        in_specs=[
            pl.BlockSpec((8, LANES), lambda j: (0, 0)),
            pl.BlockSpec((rows, TILE), lambda j: (1, j)),
            pl.BlockSpec((rows, TILE), lambda j: (1, lower(j))),
            pl.BlockSpec((rows, TILE), lambda j: (1, upper(j))),
        ],
        out_specs=[
            pl.BlockSpec((rows, TILE), lambda j: (0, lower(j))),
            pl.BlockSpec((rows, TILE), lambda j: (0, upper(j))),
            pl.BlockSpec((8, LANES), lambda j: (0, 0)),
        ],
        compiler_params=params(),
        cost_estimate=pl.CostEstimate(flops=600 * rows * tiles * TILE, bytes_accessed=12 * rows * tiles * TILE, transcendentals=0),
    )(order, keep, rx, ry)


def final_kernel(half, buf_ref, order_ref, keep_ref, rx_ref, ry_ref, last0_ref, last1_ref, out_ref):
    step = pl.program_id(0)

    @pl.when(step < half)
    def _():
        out_ref[...] = keep_ref[...] + rx_ref[...] + last0_ref[...]

    @pl.when(step >= half)
    def _():
        out_ref[...] = keep_ref[...] + ry_ref[...] + last1_ref[...]


def run_final(first, tiles, vocab, order, buf, keep, rx, ry, last0, last1):
    rows = last0.shape[0]
    half = tiles // 2
    lower = lambda j: (0, jnp.minimum(j, half - 1))
    upper = lambda j: (0, jnp.maximum(j - half, 0))
    specs = [
        pl.BlockSpec((8, LANES), lambda j: (0, 0)),
        pl.BlockSpec((rows, TILE), lambda j: (0, j)),
        pl.BlockSpec((rows, TILE), lower),
        pl.BlockSpec((rows, TILE), upper),
        pl.BlockSpec((rows, TILE), lower),
        pl.BlockSpec((rows, TILE), upper),
    ]
    body = functools.partial(final_kernel, half)
    operands = (order, keep, rx, ry, last0, last1)
    aliases = {}
    if buf is None:
        body = functools.partial(final_kernel, half, None)
    else:
        specs = [pl.BlockSpec(memory_space=pl.ANY)] + specs
        operands = (buf,) + operands
        aliases = {0: 0}
    return pl.pallas_call(
        body,
        name="finish",
        grid=(tiles,),
        out_shape=jax.ShapeDtypeStruct((rows, vocab), jnp.float32),
        in_specs=specs,
        out_specs=pl.BlockSpec((rows, TILE), lambda j: (0, first + j)),
        input_output_aliases=aliases,
        compiler_params=params(),
        cost_estimate=pl.CostEstimate(flops=600 * rows * tiles * TILE, bytes_accessed=16 * rows * tiles * TILE, transcendentals=0),
    )(*operands)


def solution(mesh):
    dp = mesh.shape['dp']
    swap = {bit: [(i, i ^ bit) for i in range(dp)] for bit in range(1, dp)}
    across = [(0, 1), (1, 0)]

    def device_fn(hid_loc, norm_w, emb_loc, teach_loc, mask_loc):
        me = lax.axis_index('dp')
        tokens, dim = hid_loc.shape
        vocab = emb_loc.shape[0]
        mask_f32 = mask_loc.astype(jnp.float32)
        count = jnp.full((8, LANES), jnp.sum(mask_f32), jnp.float32)
        tok_count = count
        for bit in range(1, dp):
            tok_count = tok_count + lax.ppermute(count, 'dp', swap[bit])
        weight = mask_f32 / tok_count[0, 0]

        normed_f32, norm_pull = jax.vjp(rms_norm, hid_loc.astype(jnp.float32), norm_w.astype(jnp.float32))
        normed = normed_f32.astype(jnp.bfloat16)
        emb_t = emb_loc.T
        mine = run_stats(normed, emb_t, teach_loc)

        blocks = normed.T.reshape(dp, dim // dp, tokens)

        def arranged(flips):
            return jnp.concatenate([lax.dynamic_index_in_dim(blocks, me ^ flip, 0, keepdims=False) for flip in flips], axis=0)

        g_own = jnp.stack([arranged((0, 4, 2, 6)), arranged((0, 2, 4, 6))])
        g_partner = jnp.stack([arranged((1, 5, 3, 7)), arranged((1, 3, 5, 7))])

        other = lax.ppermute(mine, 'tp', across)
        top = jnp.maximum(mine[0], other[0])
        mine_scale = jnp.exp(mine[0] - top)
        other_scale = jnp.exp(other[0] - top)
        sum_stu = mine[1] + other[1]
        sum_tea = mine[2] * mine_scale + other[2] * other_scale
        dot_kl = mine[3] * mine_scale + other[3] * other_scale
        kl_tok = dot_kl / sum_tea - (top + jnp.log(sum_tea)) + jnp.log(sum_stu)
        coef = jnp.stack([top, weight / sum_stu, weight / sum_tea])
        coef = jnp.broadcast_to(coef[:, :, None], (3, tokens, LANES))

        zero_token = jnp.zeros((8, LANES), jnp.float32)
        grad_part = jnp.zeros((tokens, dim), jnp.float32)
        count_chunks = len(CHUNK_TILES)
        firsts = [sum(CHUNK_TILES[:k]) for k in range(count_chunks)]
        a_token, b_token = {}, {}
        d_raw, recv, state = {}, {}, {}

        def do_a(k, grad):
            order = b_token[k - 2] if k >= 2 else zero_token
            d_raw[k], part, grad, a_token[k] = run_a(firsts[k], CHUNK_TILES[k], order, grad, coef, normed, g_partner, emb_t, teach_loc)
            recv[k] = lax.ppermute(part, 'dp', swap[1])
            return grad

        def do_b(k):
            order = a_token[min(k + 1, count_chunks - 1)]
            keep, send0, send1, b_token[k] = run_b(CHUNK_TILES[k], order, g_own, d_raw[k], recv[k])
            rx = lax.ppermute(send0, 'dp', swap[2])
            ry = lax.ppermute(send1, 'dp', swap[4])
            state[k] = (keep, rx, ry)

        grad_part = do_a(0, grad_part)
        for k in range(1, count_chunks):
            grad_part = do_a(k, grad_part)
            do_b(k - 1)
        do_b(count_chunks - 1)

        order = b_token[count_chunks - 1]
        for k in range(count_chunks):
            last0, last1, order = run_relay(CHUNK_TILES[k], order, *state[k])
            last0 = lax.ppermute(last0, 'dp', swap[4])
            last1 = lax.ppermute(last1, 'dp', swap[2])
            state[k] += (last0, last1)

        grad_other = lax.ppermute(grad_part, 'tp', across)
        grad_normed = grad_part + grad_other
        grad_hid, grad_scale = norm_pull(grad_normed)
        loss_val, grad_w = lax.psum((jnp.sum(weight * kl_tok), grad_scale), 'dp')

        grad_emb = None
        for k in range(count_chunks):
            order = order if k < count_chunks - 3 else jnp.broadcast_to(grad_w[:LANES], (8, LANES))
            grad_emb = run_final(firsts[k], CHUNK_TILES[k], vocab, order, grad_emb, *state[k])
        return loss_val, grad_hid.astype(jnp.bfloat16), grad_emb.T, grad_w

    return jax.shard_map(device_fn, mesh=mesh, in_specs=(P('dp', None), P(None), P('tp', None), P('dp', 'tp'), P('dp')), out_specs=(P(), P('dp', None), P('tp', 'dp'), P(None)), check_vma=False)
```

```python
import functools

import jax
import jax.numpy as jnp
from jax import lax
from jax.experimental import pallas as pl
from jax.experimental.pallas import tpu as pltpu
from jax.sharding import PartitionSpec as P


SOFT_CAP = 30.0
NORM_EPS = 1e-6
LOG2E = 1.4426950408889634
TILE = 512
STRIP = 256
SUB = 16
LANES = 128
CHUNK_TILES = (2, 2, 4, 8, 10, 10, 8, 4)
LOWEST = -3.0e38
VMEM_LIMIT = 60 * 1024 * 1024


def rms_norm(hid_f32, scale_f32):
    inv_rms = lax.rsqrt(jnp.mean(hid_f32 * hid_f32, axis=-1, keepdims=True) + NORM_EPS)
    return hid_f32 * inv_rms * (1.0 + scale_f32)


def params():
    return pltpu.CompilerParams(dimension_semantics=("arbitrary",), vmem_limit_bytes=VMEM_LIMIT)


def stats_kernel(steps, g_ref, e_ref, t_ref, out_ref, u_ref, m_ref, zs_ref, zt_ref, kl_ref):
    step = pl.program_id(0)

    @pl.when(step == 0)
    def _():
        m_ref[...] = jnp.full(m_ref.shape, LOWEST, jnp.float32)
        zs_ref[...] = jnp.zeros_like(zs_ref)
        zt_ref[...] = jnp.zeros_like(zt_ref)
        kl_ref[...] = jnp.zeros_like(kl_ref)

    groups = TILE // LANES
    tokens = g_ref.shape[0]

    def logits(strip):
        return jnp.dot(g_ref[pl.ds(strip * STRIP, STRIP), :], e_ref[...], preferred_element_type=jnp.float32)

    raw = logits(0)
    for strip in range(tokens // STRIP):
        following = logits(strip + 1) if (strip + 1) * STRIP < tokens else None
        for sub in range(STRIP // SUB):
            rows = pl.ds(strip * STRIP + sub * SUB, SUB)
            block = raw[sub * SUB:(sub + 1) * SUB]
            tea = t_ref[rows, :].astype(jnp.float32)
            parts = [tea[:, k * LANES:(k + 1) * LANES] for k in range(groups)]
            top = m_ref[rows, :]
            old = top
            for part in parts:
                top = jnp.maximum(top, part)
            decay = jnp.exp2((old - top) * LOG2E)
            zs = zs_ref[rows, :]
            zt = zt_ref[rows, :] * decay
            kl = kl_ref[rows, :] * decay
            for k, part in enumerate(parts):
                tanh_val = jnp.tanh(block[:, k * LANES:(k + 1) * LANES] * (1.0 / SOFT_CAP))
                u_ref[rows, k * LANES:(k + 1) * LANES] = tanh_val
                zs = zs + jnp.exp2(tanh_val * (SOFT_CAP * LOG2E))
                ex = jnp.exp2((part - top) * LOG2E)
                zt = zt + ex
                kl = kl + ex * (part - SOFT_CAP * tanh_val)
            m_ref[rows, :] = top
            zs_ref[rows, :] = zs
            zt_ref[rows, :] = zt
            kl_ref[rows, :] = kl
        raw = following

    @pl.when(step == steps - 1)
    def _():
        lane_max = m_ref[...]
        top = jnp.max(lane_max, axis=-1, keepdims=True)
        decay = jnp.exp2((lane_max - top) * LOG2E)
        zs = jnp.sum(zs_ref[...], axis=-1, keepdims=True)
        zt = jnp.sum(zt_ref[...] * decay, axis=-1, keepdims=True)
        kl = jnp.sum(kl_ref[...] * decay, axis=-1, keepdims=True)
        lane = lax.broadcasted_iota(jnp.int32, lane_max.shape, 1)
        packed = jnp.where(lane == 0, top, jnp.where(lane == 1, zs, jnp.where(lane == 2, zt, kl)))
        out_ref[...] = packed.T[:8, :]


def run_stats(normed, emb_t, teach):
    tokens, dim = normed.shape
    vocab = emb_t.shape[1]
    steps = vocab // TILE
    return pl.pallas_call(
        functools.partial(stats_kernel, steps),
        name="stats",
        grid=(steps,),
        out_shape=[
            jax.ShapeDtypeStruct((8, tokens), jnp.float32),
            jax.ShapeDtypeStruct((tokens, vocab), jnp.float32),
        ],
        in_specs=[
            pl.BlockSpec((tokens, dim), lambda j: (0, 0)),
            pl.BlockSpec((dim, TILE), lambda j: (0, j)),
            pl.BlockSpec((tokens, TILE), lambda j: (0, j)),
        ],
        out_specs=[
            pl.BlockSpec((8, tokens), lambda j: (0, 0)),
            pl.BlockSpec((tokens, TILE), lambda j: (0, j)),
        ],
        scratch_shapes=[pltpu.VMEM((tokens, LANES), jnp.float32)] * 4,
        compiler_params=params(),
        cost_estimate=pl.CostEstimate(flops=2 * tokens * dim * vocab, bytes_accessed=2 * vocab * (3 * tokens + dim), transcendentals=3 * tokens * vocab),
    )(normed, emb_t, teach)


def a_kernel(chained, *refs):
    if chained:
        order_ref, prev_ref, *refs = refs
    coef_ref, gp_ref, e_ref, t_ref, u_ref, dr_ref, pp_ref, dg_ref, tok_ref = refs

    @pl.when(pl.program_id(0) == 0)
    def _():
        dg_ref[...] = prev_ref[...] if chained else jnp.zeros_like(dg_ref)
        tok_ref[...] = jnp.zeros_like(tok_ref)

    groups = TILE // LANES
    tokens = u_ref.shape[0]
    for strip in range(tokens // STRIP):
        for sub in range(STRIP // SUB):
            rows = pl.ds(strip * STRIP + sub * SUB, SUB)
            top = coef_ref[0, rows, :]
            stu_w = coef_ref[1, rows, :]
            tea_w = coef_ref[2, rows, :]
            for k in range(groups):
                cols = slice(k * LANES, (k + 1) * LANES)
                tanh_val = u_ref[rows, cols]
                stu = jnp.exp2(tanh_val * (SOFT_CAP * LOG2E)) * stu_w
                soft = jnp.exp2((t_ref[rows, cols].astype(jnp.float32) - top) * LOG2E) * tea_w
                d_raw = (stu - soft) * (1.0 - tanh_val * tanh_val)
                dr_ref[rows, cols] = d_raw.astype(jnp.bfloat16)
        part = pl.ds(strip * STRIP, STRIP)
        dg_ref[part, :] += lax.dot_general(dr_ref[part, :], e_ref[...], (((1,), (1,)), ((), ())), preferred_element_type=jnp.float32)
    pp_ref[...] = jnp.dot(gp_ref[0], dr_ref[...], preferred_element_type=jnp.float32)


def run_a(first, tiles, chain, coef, g_partner, emb_t, teach, tanh_all):
    tokens = teach.shape[0]
    dim = emb_t.shape[0]
    half = tiles // 2
    width = tiles * TILE
    rows = g_partner.shape[1]
    return pl.pallas_call(
        functools.partial(a_kernel, bool(chain)),
        name="dlogits",
        grid=(tiles,),
        out_shape=[
            jax.ShapeDtypeStruct((tokens, width), jnp.bfloat16),
            jax.ShapeDtypeStruct((rows, width), jnp.float32),
            jax.ShapeDtypeStruct((tokens, dim), jnp.float32),
            jax.ShapeDtypeStruct((8, LANES), jnp.float32),
        ],
        in_specs=[
            pl.BlockSpec((8, LANES), lambda j: (0, 0)),
            pl.BlockSpec((tokens, dim), lambda j: (0, 0)),
        ][:len(chain)] + [
            pl.BlockSpec((3, tokens, LANES), lambda j: (0, 0, 0)),
            pl.BlockSpec((1, rows, tokens), lambda j: (j // half, 0, 0)),
            pl.BlockSpec((dim, TILE), lambda j: (0, first + j)),
            pl.BlockSpec((tokens, TILE), lambda j: (0, first + j)),
            pl.BlockSpec((tokens, TILE), lambda j: (0, first + j)),
        ],
        out_specs=[
            pl.BlockSpec((tokens, TILE), lambda j: (0, j)),
            pl.BlockSpec((rows, TILE), lambda j: (0, j)),
            pl.BlockSpec((tokens, dim), lambda j: (0, 0)),
            pl.BlockSpec((8, LANES), lambda j: (0, 0)),
        ],
        compiler_params=params(),
        cost_estimate=pl.CostEstimate(flops=4 * tokens * dim * width, bytes_accessed=12 * tokens * width, transcendentals=2 * tokens * width),
    )(*chain, coef, g_partner, emb_t, teach, tanh_all)


def b_kernel(half, order_ref, go_ref, dr_ref, r_ref, keep_ref, send0_ref, send1_ref, tok_ref):
    step = pl.program_id(0)
    total = jnp.dot(go_ref[0], dr_ref[...], preferred_element_type=jnp.float32) + r_ref[...]
    mid = keep_ref.shape[0]
    keep_ref[...] = total[:mid]

    @pl.when(step == 0)
    def _():
        tok_ref[...] = jnp.zeros_like(tok_ref)

    @pl.when(step < half)
    def _():
        send0_ref[...] = total[mid:]

    @pl.when(step >= half)
    def _():
        send1_ref[...] = total[mid:]


def run_b(tiles, order, g_own, d_raw, recv):
    tokens = d_raw.shape[0]
    rows = g_own.shape[1]
    half = tiles // 2
    width = tiles * TILE
    lower = lambda j: (0, jnp.minimum(j, half - 1))
    upper = lambda j: (0, jnp.maximum(j - half, 0))
    return pl.pallas_call(
        functools.partial(b_kernel, half),
        name="own_half",
        grid=(tiles,),
        out_shape=[
            jax.ShapeDtypeStruct((rows // 2, width), jnp.float32),
            jax.ShapeDtypeStruct((rows // 2, width // 2), jnp.float32),
            jax.ShapeDtypeStruct((rows // 2, width // 2), jnp.float32),
            jax.ShapeDtypeStruct((8, LANES), jnp.float32),
        ],
        in_specs=[
            pl.BlockSpec((8, LANES), lambda j: (0, 0)),
            pl.BlockSpec((1, rows, tokens), lambda j: (j // half, 0, 0)),
            pl.BlockSpec((tokens, TILE), lambda j: (0, j)),
            pl.BlockSpec((rows, TILE), lambda j: (0, j)),
        ],
        out_specs=[
            pl.BlockSpec((rows // 2, TILE), lambda j: (0, j)),
            pl.BlockSpec((rows // 2, TILE), lower),
            pl.BlockSpec((rows // 2, TILE), upper),
            pl.BlockSpec((8, LANES), lambda j: (0, 0)),
        ],
        compiler_params=params(),
        cost_estimate=pl.CostEstimate(flops=2 * tokens * rows * width, bytes_accessed=width * (2 * tokens + 8 * rows), transcendentals=0),
    )(order, g_own, d_raw, recv)


def relay_kernel(half, order_ref, keep_ref, rx_ref, ry_ref, last0_ref, last1_ref, tok_ref):
    step = pl.program_id(0)

    @pl.when(step == 0)
    def _():
        tok_ref[...] = jnp.zeros_like(tok_ref)

    @pl.when(step < half)
    def _():
        last0_ref[...] = keep_ref[...] + rx_ref[...]

    @pl.when(step >= half)
    def _():
        last1_ref[...] = keep_ref[...] + ry_ref[...]


def run_relay(tiles, order, keep, rx, ry):
    rows = keep.shape[0] // 2
    half = tiles // 2
    width = half * TILE
    lower = lambda j: jnp.minimum(j, half - 1)
    upper = lambda j: jnp.maximum(j - half, 0)
    return pl.pallas_call(
        functools.partial(relay_kernel, half),
        name="relay",
        grid=(tiles,),
        out_shape=[
            jax.ShapeDtypeStruct((rows, width), jnp.float32),
            jax.ShapeDtypeStruct((rows, width), jnp.float32),
            jax.ShapeDtypeStruct((8, LANES), jnp.float32),
        ],
        in_specs=[
            pl.BlockSpec((8, LANES), lambda j: (0, 0)),
            pl.BlockSpec((rows, TILE), lambda j: (1, j)),
            pl.BlockSpec((rows, TILE), lambda j: (1, lower(j))),
            pl.BlockSpec((rows, TILE), lambda j: (1, upper(j))),
        ],
        out_specs=[
            pl.BlockSpec((rows, TILE), lambda j: (0, lower(j))),
            pl.BlockSpec((rows, TILE), lambda j: (0, upper(j))),
            pl.BlockSpec((8, LANES), lambda j: (0, 0)),
        ],
        compiler_params=params(),
        cost_estimate=pl.CostEstimate(flops=600 * rows * tiles * TILE, bytes_accessed=12 * rows * tiles * TILE, transcendentals=0),
    )(order, keep, rx, ry)


def final_kernel(half, buf_ref, order_ref, keep_ref, rx_ref, ry_ref, last0_ref, last1_ref, out_ref):
    step = pl.program_id(0)

    @pl.when(step < half)
    def _():
        out_ref[...] = keep_ref[...] + rx_ref[...] + last0_ref[...]

    @pl.when(step >= half)
    def _():
        out_ref[...] = keep_ref[...] + ry_ref[...] + last1_ref[...]


def run_final(first, tiles, vocab, order, buf, keep, rx, ry, last0, last1):
    rows = last0.shape[0]
    half = tiles // 2
    lower = lambda j: (0, jnp.minimum(j, half - 1))
    upper = lambda j: (0, jnp.maximum(j - half, 0))
    specs = [
        pl.BlockSpec((8, LANES), lambda j: (0, 0)),
        pl.BlockSpec((rows, TILE), lambda j: (0, j)),
        pl.BlockSpec((rows, TILE), lower),
        pl.BlockSpec((rows, TILE), upper),
        pl.BlockSpec((rows, TILE), lower),
        pl.BlockSpec((rows, TILE), upper),
    ]
    body = functools.partial(final_kernel, half)
    operands = (order, keep, rx, ry, last0, last1)
    aliases = {}
    if buf is None:
        body = functools.partial(final_kernel, half, None)
    else:
        specs = [pl.BlockSpec(memory_space=pl.ANY)] + specs
        operands = (buf,) + operands
        aliases = {0: 0}
    return pl.pallas_call(
        body,
        name="finish",
        grid=(tiles,),
        out_shape=jax.ShapeDtypeStruct((rows, vocab), jnp.float32),
        in_specs=specs,
        out_specs=pl.BlockSpec((rows, TILE), lambda j: (0, first + j)),
        input_output_aliases=aliases,
        compiler_params=params(),
        cost_estimate=pl.CostEstimate(flops=600 * rows * tiles * TILE, bytes_accessed=16 * rows * tiles * TILE, transcendentals=0),
    )(*operands)


def plan():
    chunks = len(CHUNK_TILES)
    steps = [("dlog", 0), ("own", 0), ("dlog", 1), ("own", 1)]
    for k in range(2, chunks):
        steps.append(("dlog", k))
        if k >= 3:
            steps.append(("own", k - 1))
            steps.append(("relay", k - 3))
    steps.append(("own", chunks - 1))
    return steps + [("relay", k) for k in range(chunks - 3, chunks)]


def solution(mesh):
    dp = mesh.shape['dp']
    swap = {bit: [(i, i ^ bit) for i in range(dp)] for bit in range(1, dp)}
    across = [(0, 1), (1, 0)]

    def device_fn(hid_loc, norm_w, emb_loc, teach_loc, mask_loc):
        me = lax.axis_index('dp')
        tokens, dim = hid_loc.shape
        vocab = emb_loc.shape[0]
        mask_f32 = mask_loc.astype(jnp.float32)
        count = jnp.full((8, LANES), jnp.sum(mask_f32), jnp.float32)
        tok_count = count
        for bit in range(1, dp):
            tok_count = tok_count + lax.ppermute(count, 'dp', swap[bit])
        weight = mask_f32 / tok_count[0, 0]

        normed_f32, norm_pull = jax.vjp(rms_norm, hid_loc.astype(jnp.float32), norm_w.astype(jnp.float32))
        normed = normed_f32.astype(jnp.bfloat16)
        emb_t = emb_loc.T
        mine, tanh_all = run_stats(normed, emb_t, teach_loc)

        blocks = normed.T.reshape(dp, dim // dp, tokens)

        def arranged(flips):
            return jnp.concatenate([lax.dynamic_index_in_dim(blocks, me ^ flip, 0, keepdims=False) for flip in flips], axis=0)

        g_own = jnp.stack([arranged((0, 4, 2, 6)), arranged((0, 2, 4, 6))])
        g_partner = jnp.stack([arranged((1, 5, 3, 7)), arranged((1, 3, 5, 7))])

        other = lax.ppermute(mine, 'tp', across)
        top = jnp.maximum(mine[0], other[0])
        mine_scale = jnp.exp(mine[0] - top)
        other_scale = jnp.exp(other[0] - top)
        sum_stu = mine[1] + other[1]
        sum_tea = mine[2] * mine_scale + other[2] * other_scale
        dot_kl = mine[3] * mine_scale + other[3] * other_scale
        kl_tok = dot_kl / sum_tea - (top + jnp.log(sum_tea)) + jnp.log(sum_stu)
        coef = jnp.stack([top, weight / sum_stu, weight / sum_tea])
        coef = jnp.broadcast_to(coef[:, :, None], (3, tokens, LANES))

        count_chunks = len(CHUNK_TILES)
        firsts = [sum(CHUNK_TILES[:k]) for k in range(count_chunks)]
        last = None
        grad_part = None
        d_raw, recv, state = {}, {}, {}
        for verb, k in plan():
            tiles = CHUNK_TILES[k]
            if verb == "dlog":
                chain = () if last is None else (last, grad_part)
                d_raw[k], part, grad_part, last = run_a(firsts[k], tiles, chain, coef, g_partner, emb_t, teach_loc, tanh_all)
            elif verb == "own":
                keep, send0, send1, last = run_b(tiles, last, g_own, d_raw[k], recv[k])
            else:
                last0, last1, last = run_relay(tiles, last, *state[k])
            if verb == "dlog":
                recv[k] = lax.ppermute(part, 'dp', swap[1])
            elif verb == "own":
                rx = lax.ppermute(send0, 'dp', swap[2])
                ry = lax.ppermute(send1, 'dp', swap[4])
                state[k] = (keep, rx, ry)
            else:
                last0 = lax.ppermute(last0, 'dp', swap[4])
                last1 = lax.ppermute(last1, 'dp', swap[2])
                state[k] += (last0, last1)

        grad_other = lax.ppermute(grad_part, 'tp', across)
        grad_normed = grad_part + grad_other
        grad_hid, grad_scale = norm_pull(grad_normed)
        loss_val, grad_w = lax.psum((jnp.sum(weight * kl_tok), grad_scale), 'dp')

        grad_emb = None
        for k in range(count_chunks):
            order = last if k < count_chunks - 3 else jnp.broadcast_to(grad_w[:LANES], (8, LANES))
            grad_emb = run_final(firsts[k], CHUNK_TILES[k], vocab, order, grad_emb, *state[k])
        return loss_val, grad_hid.astype(jnp.bfloat16), grad_emb.T, grad_w

    return jax.shard_map(device_fn, mesh=mesh, in_specs=(P('dp', None), P(None), P('tp', None), P('dp', 'tp'), P('dp')), out_specs=(P(), P('dp', None), P('tp', 'dp'), P(None)), check_vma=False)
```
